32 devices in a mesh: own: 8 (over z, y), blk: 4 (over x, core).
Axes of the slice: x: 2, y: 2, z: 4, core: 2. Of those that a mesh axis runs over, the one named last changes fastest.
Arguments:
- points: bfloat16 [64, 4096], P(None, ('own', 'blk')), may hold values from -6 to 6
- solution_field: float32 [33, 4096], P(None, ('own', 'blk')), may hold values from -6 to 6
- residual: float32 [33, 4096], P(None, ('own', 'blk')), may hold values from -12 to 12
- direction: float32 [33, 4096], P(None, ('own', 'blk')), may hold values from -12 to 12
Outputs:
- solution_next: float32 [33, 4096], P(None, ('own', 'blk'))
- residual_next: float32 [33, 4096], P(None, ('own', 'blk'))
- direction_next: float32 [33, 4096], P(None, ('own', 'blk'))
The draws below stay inside these ranges and needn't reach their ends.
All inputs are finite; a program needn't handle non-finite values.
Results may differ from the reference program's by a relative error of at most 0.0027.
Values may be sent and summed in bfloat16 or wider, within the bound.
A program may use at most 64 MiB of HBM per device.

```python
import math
import jax
import jax.numpy as jnp
from jax import lax

DIM = 64
RHS = 33
POINTS = 4096


def rising_field(key):
    index = jnp.arange(POINTS, dtype=jnp.float32)
    scale = 1.0 + 2.0 * index / (POINTS - 1)
    base = jax.random.truncated_normal(key, -4.0, 4.0, (RHS, POINTS), jnp.float32)
    return base * scale[None, :]


def draw_residual(key, part):
    return rising_field(jax.random.fold_in(key, 11))


def draw_direction(key, part):
    return rising_field(jax.random.fold_in(key, 23))


def levels(key, shape, shards, smallest, largest):
    loudness = 1.0
    for axis_at, shards_of in shards:
        draws = jax.random.uniform(jax.random.fold_in(jax.random.fold_in(key, 6), axis_at), (shards_of,), jnp.float32, smallest / len(shards), largest / len(shards))
        loudness = loudness * jnp.repeat(jnp.exp(draws), shape[axis_at] // shards_of).reshape((-1,) + (1,) * (len(shape) - 1 - axis_at))
    return loudness


def normal_values(own_key, shape, scale, most, pieces=(), kind=jnp.bfloat16):
    level = levels(own_key, shape, pieces, -0.22, 0.18) if pieces else 1.0
    array = jax.random.normal(own_key, shape, jnp.float32) * scale * level
    return jnp.minimum(jnp.maximum(array, -most), most).astype(kind)


def setup_inputs(seed: int = 0) -> dict:
    key_list = jax.random.split(jax.random.key(seed), 5)
    return {
        "points": normal_values(key_list[0], (DIM, POINTS), 1.0, 6.0, ((1, 32),)),
        "solution_field": normal_values(key_list[1], (RHS, POINTS), 1.0, 6.0, ((1, 32),), jnp.float32),
        "residual": draw_residual(jax.random.fold_in(key_list[4], 71), 0),
        "direction": draw_direction(jax.random.fold_in(key_list[4], 71), 0),
    }


amplitude = 1.0
decay_rate = 1.0 / 16.0
noise_level = 0.5


def tile_products(row_blocks, row_norms, columns, dirs):
    col_norms = jnp.sum(jnp.square(columns.astype(jnp.float32)), axis=0)

    def single(pair):
        rows, norms = pair
        inner = lax.dot_general(rows, columns, (((0,), (0,)), ((), ())), preferred_element_type=jnp.float32)
        dist = jnp.maximum(norms[:, None] + col_norms[None, :] - 2.0 * inner, 0.0)
        kern = (amplitude * jnp.exp(-decay_rate * dist)).astype(jnp.bfloat16)
        return lax.dot_general(dirs, kern, (((1,), (1,)), ((), ())), preferred_element_type=jnp.float32)

    return lax.map(single, (row_blocks, row_norms))


def reference(points, solution_field, residual, direction):
    width = points.shape[1]
    size = math.gcd(width, 512)
    count = width // size
    blocks = points.reshape(points.shape[0], count, size).transpose(1, 0, 2)
    norms = jnp.sum(jnp.square(blocks.astype(jnp.float32)), axis=1)
    dir_low = direction.astype(jnp.bfloat16)
    prods = tile_products(blocks, norms, points, dir_low)
    image = prods.transpose(1, 0, 2).reshape(direction.shape[0], width) + noise_level * direction
    rr_sum = jnp.sum(residual * residual, axis=1)
    pq_sum = jnp.sum(direction * image, axis=1)
    alpha = (rr_sum / pq_sum)[:, None]
    solution_next = solution_field + alpha * direction
    residual_next = residual - alpha * image
    new_sum = jnp.sum(residual_next * residual_next, axis=1)
    direction_next = residual_next + (new_sum / rr_sum)[:, None] * direction
    return solution_next, residual_next, direction_next
```

```python
import functools
import math

import jax
import jax.numpy as jnp
from jax import lax
from jax.experimental import pallas as pl
from jax.experimental.pallas import tpu as pltpu
from jax.sharding import PartitionSpec as P

amplitude = 1.0
decay_rate = 1.0 / 16.0
noise_level = 0.5

LOG2E = math.log2(math.e)
MESH = pl.DeviceIdType.MESH


def split_own(n_own, n_blk):
    for low in range(1, n_own + 1):
        if n_own % low == 0 and low * n_blk > n_own // low:
            return low
    return n_own


def wait_bytes(ref, sem):
    pltpu.make_async_copy(ref, ref, sem).wait()


def kernel(n_own, n_blk, low, points_ref, solution_ref, residual_ref, direction_ref,
           solution_out, residual_out, direction_out,
           rows_ref, cols_ref, norms_ref, acc_ref, part_ref, back_ref, sums_ref,
           row_send, row_recv, col_send, col_recv, part_send, part_recv, sum_send, sum_recv):
    high = n_own // low
    n_row, n_col = low * n_blk, high
    dim, width = points_ref.shape
    rhs = direction_ref.shape[0]
    own, blk = lax.axis_index("own"), lax.axis_index("blk")
    h, l = own // low, own % low
    r = l * n_blk + blk
    scale = decay_rate * LOG2E

    def row_peer(k):
        other = (r + k) % n_row
        return (h * low + other // n_blk, other % n_blk)

    def col_peer(k):
        return (((h + k) % high) * low + l, blk)

    barrier = pltpu.get_barrier_semaphore()
    for k in range(1, n_col):
        pl.semaphore_signal(barrier, inc=1, device_id=col_peer(k), device_id_type=MESH)
    for k in range(1, n_row):
        pl.semaphore_signal(barrier, inc=1, device_id=row_peer(k), device_id_type=MESH)

    cols_ref[0, :dim, :] = points_ref[...]
    cols_ref[0, dim:, :] = jnp.zeros(cols_ref.shape[1:], jnp.bfloat16)[dim:]
    cols_ref[0, dim:dim + rhs, :] = direction_ref[...].astype(jnp.bfloat16)
    rows_ref[:, :width] = points_ref[...]

    pl.semaphore_wait(barrier, n_row + n_col - 2)

    col_copies = []
    for k in range(1, n_col):
        slot = n_col - k
        copy = pltpu.make_async_remote_copy(
            src_ref=cols_ref.at[0], dst_ref=cols_ref.at[slot], send_sem=col_send.at[slot],
            recv_sem=col_recv.at[slot], device_id=col_peer(k), device_id_type=MESH)
        copy.start()
        col_copies.append(copy)
    row_copies = []
    for k in range(1, n_row):
        slot = n_row - k
        copy = pltpu.make_async_remote_copy(
            src_ref=points_ref, dst_ref=rows_ref.at[:, pl.ds(slot * width, width)],
            send_sem=row_send.at[slot], recv_sem=row_recv.at[slot],
            device_id=row_peer(k), device_id_type=MESH)
        copy.start()
        row_copies.append(copy)

    diag = (lax.broadcasted_iota(jnp.int32, (rhs, width), 0)
            == lax.broadcasted_iota(jnp.int32, (rhs, width), 1))

    def to_row(products):
        column = jnp.sum(products, axis=1, keepdims=True)
        return jnp.sum(jnp.where(diag, column, 0.0), axis=0, keepdims=True)

    def to_column(row):
        return jnp.sum(jnp.where(diag, row, 0.0), axis=1, keepdims=True)

    residual = residual_ref[...]
    direction = direction_ref[...]
    sums_ref[0, 0:1, :] = to_row(residual * residual)

    for copy in row_copies:
        copy.wait_recv()
    chunk = math.gcd(n_row * width, 2 * width)
    n_chunk = n_row * width // chunk
    for c in range(n_chunk):
        wide = rows_ref[:, c * chunk:(c + 1) * chunk].astype(jnp.float32)
        norms_ref[:, c * chunk:(c + 1) * chunk] = jnp.sum(wide * wide, axis=0, keepdims=True) * scale

    part_copies = []
    per = chunk // width
    for k in range(n_col):
        if k > 0:
            wait_bytes(cols_ref.at[k], col_recv.at[k])
        wide = cols_ref[k, :dim, :].astype(jnp.float32).T
        col_norms = jnp.sum(wide * wide, axis=1, keepdims=True) * scale
        turned = wide.astype(jnp.bfloat16)
        dirs = cols_ref[k, dim:, :]
        for c in range(n_chunk):
            at = slice(c * chunk, (c + 1) * chunk)
            inner = jnp.dot(turned, rows_ref[:, at], preferred_element_type=jnp.float32)
            power = jnp.minimum(inner * (2.0 * scale) - norms_ref[:, at] - col_norms, 0.0)
            kern = (amplitude * jnp.exp2(power)).astype(jnp.bfloat16)
            value = jnp.dot(dirs, kern, preferred_element_type=jnp.float32)
            if k > 0:
                value += acc_ref[:, at]
            if k < n_col - 1:
                acc_ref[:, at] = value
                continue
            for j in range(per):
                to = c * per + j
                piece = value[:, j * width:(j + 1) * width]
                if to == 0:
                    acc_ref[:, :width] = piece
                    continue
                part_ref[to] = piece.astype(jnp.bfloat16)
                slot = n_row - to
                copy = pltpu.make_async_remote_copy(
                    src_ref=part_ref.at[to], dst_ref=back_ref.at[slot],
                    send_sem=part_send.at[slot], recv_sem=part_recv.at[slot],
                    device_id=row_peer(to), device_id_type=MESH)
                copy.start()
                part_copies.append(copy)

    image = acc_ref[:, :width]
    for k in range(1, n_row):
        wait_bytes(back_ref.at[k], part_recv.at[k])
        image += back_ref[k].astype(jnp.float32)
    image = image[:rhs] + noise_level * direction

    sums_ref[0, 1:2, :] = to_row(direction * image)
    sums_ref[0, 2:3, :] = to_row(residual * image)
    sums_ref[0, 3:4, :] = to_row(image * image)
    n_all = n_own * n_blk

    def send_sums(k, carry):
        peer = ((own + k // n_blk) % n_own, (blk + k % n_blk) % n_blk)
        slot = ((n_own - k // n_blk) % n_own) * n_blk + (n_blk - k % n_blk) % n_blk
        pltpu.make_async_remote_copy(
            src_ref=sums_ref.at[0], dst_ref=sums_ref.at[slot], send_sem=sum_send,
            recv_sem=sum_recv, device_id=peer, device_id_type=MESH).start()
        return carry

    lax.fori_loop(1, n_all, send_sums, 0)

    for copy in col_copies + row_copies + part_copies:
        copy.wait_send()
    wait_bytes(sums_ref.at[pl.ds(1, n_all - 1)], sum_send)
    wait_bytes(sums_ref.at[pl.ds(1, n_all - 1)], sum_recv)
    total = jnp.sum(sums_ref[...], axis=0)
    rr, pq, rq, qq = (total[i:i + 1] for i in range(4))
    alpha_row = rr / pq
    new_sum = rr - 2.0 * alpha_row * rq + alpha_row * alpha_row * qq
    alpha = to_column(alpha_row)
    beta = to_column(new_sum / rr)
    residual_next = residual - alpha * image
    residual_out[...] = residual_next
    solution_out[...] = solution_ref[...] + alpha * direction
    direction_out[...] = residual_next + beta * direction


def local(n_own, n_blk, points, solution_field, residual, direction):
    low = split_own(n_own, n_blk)
    n_row, n_col = low * n_blk, n_own // low
    dim, width = points.shape
    rhs = direction.shape[0]
    padded = -(-rhs // 16) * 16
    vmem = pl.BlockSpec(memory_space=pltpu.VMEM)
    out = jax.ShapeDtypeStruct(direction.shape, jnp.float32)
    dma = pltpu.SemaphoreType.DMA
    return pl.pallas_call(
        functools.partial(kernel, n_own, n_blk, low),
        out_shape=(out, out, out),
        in_specs=[vmem] * 4,
        out_specs=(vmem,) * 3,
        scratch_shapes=[
            pltpu.VMEM((dim, n_row * width), jnp.bfloat16),
            pltpu.VMEM((n_col, dim + padded, width), jnp.bfloat16),
            pltpu.VMEM((1, n_row * width), jnp.float32),
            pltpu.VMEM((padded, n_row * width), jnp.float32),
            pltpu.VMEM((n_row, padded, width), jnp.bfloat16),
            pltpu.VMEM((n_row, padded, width), jnp.bfloat16),
            pltpu.VMEM((n_own * n_blk, 4, width), jnp.float32),
            dma((n_row,)), dma((n_row,)), dma((n_col,)), dma((n_col,)),
            dma((n_row,)), dma((n_row,)), dma, dma,
        ],
        compiler_params=pltpu.CompilerParams(collective_id=0, has_side_effects=True),
    )(points, solution_field, residual, direction)


def solution(mesh):
    spec = P(None, ("own", "blk"))
    body = functools.partial(local, mesh.shape["own"], mesh.shape["blk"])
    return jax.shard_map(body, mesh=mesh, in_specs=(spec,) * 4, out_specs=(spec,) * 3, check_vma=False)
```

```python
import functools
import math

import jax
import jax.numpy as jnp
from jax import lax
from jax.experimental import pallas as pl
from jax.experimental.pallas import tpu as pltpu
from jax.sharding import PartitionSpec as P

amplitude = 1.0
decay_rate = 1.0 / 16.0
noise_level = 0.5

LOG2E = math.log2(math.e)
MESH = pl.DeviceIdType.MESH


def split_own(n_own, n_blk):
    for low in range(1, n_own + 1):
        if n_own % low == 0 and low * n_blk > n_own // low:
            return low
    return n_own


def wait_bytes(ref, sem):
    pltpu.make_async_copy(ref, ref, sem).wait()


def kernel(n_own, n_blk, low, points_hbm, residual_hbm, direction_hbm, image_out, alpha_out, beta_out,
           points_ref, residual_ref, direction_ref, load_sem, rows_ref, cols_ref, norms_ref, acc_ref, part_ref, back_ref, sums_ref, square_ref,
           row_send, row_recv, col_send, col_recv, part_send, part_recv, sum_send, sum_recv):
    high = n_own // low
    n_row, n_col = low * n_blk, high
    dim, width = points_ref.shape
    rhs = direction_ref.shape[0]
    loads = [
        pltpu.make_async_copy(points_hbm, points_ref, load_sem.at[0]),
        pltpu.make_async_copy(direction_hbm, direction_ref, load_sem.at[1]),
        pltpu.make_async_copy(residual_hbm, residual_ref, load_sem.at[2]),
    ]
    for load in loads:
        load.start()
    own, blk = lax.axis_index("own"), lax.axis_index("blk")
    h, l = lax.div(own, low), lax.rem(own, low)
    r = l * n_blk + blk
    scale = decay_rate * LOG2E

    def row_peer(k):
        other = lax.rem(r + k, n_row)
        return (h * low + lax.div(other, n_blk), lax.rem(other, n_blk))

    paired = n_col & (n_col - 1) == 0

    def col_peer(k):
        if not paired:
            return (lax.rem(h + k, high) * low + l, blk)
        other, bit = h, 1
        while bit <= k:
            if k & bit:
                other = other + bit - 2 * bit * lax.rem(lax.div(h, bit), 2)
            bit *= 2
        return (other * low + l, blk)

    barrier = pltpu.get_barrier_semaphore()
    for k in range(1, n_col):
        pl.semaphore_signal(barrier, inc=1, device_id=col_peer(k), device_id_type=MESH)
    for k in range(1, n_row):
        pl.semaphore_signal(barrier, inc=1, device_id=row_peer(k), device_id_type=MESH)

    for load in loads:
        load.wait()
    cols_ref[0, :dim, :] = points_ref[...]
    cols_ref[0, dim:, :] = jnp.zeros(cols_ref.shape[1:], jnp.bfloat16)[dim:]
    cols_ref[0, dim:dim + rhs, :] = direction_ref[...].astype(jnp.bfloat16)
    rows_ref[:, :width] = points_ref[...]

    pl.semaphore_wait(barrier, n_row + n_col - 2)

    col_copies = []
    for k in reversed(range(1, n_col)):
        slot = k if paired else n_col - k
        copy = pltpu.make_async_remote_copy(
            src_ref=cols_ref.at[0], dst_ref=cols_ref.at[slot], send_sem=col_send.at[slot],
            recv_sem=col_recv.at[slot], device_id=col_peer(k), device_id_type=MESH)
        copy.start()
        col_copies.append(copy)
    row_copies = []
    for k in range(1, n_row):
        slot = n_row - k
        copy = pltpu.make_async_remote_copy(
            src_ref=points_ref, dst_ref=rows_ref.at[:, pl.ds(slot * width, width)],
            send_sem=row_send.at[slot], recv_sem=row_recv.at[slot],
            device_id=row_peer(k), device_id_type=MESH)
        copy.start()
        row_copies.append(copy)

    row_at = lax.broadcasted_iota(jnp.int32, (rhs, width), 0)
    lane_at = lax.broadcasted_iota(jnp.int32, (rhs, width), 1)
    n_all = n_own * n_blk

    def place(i, count):
        packed = count * rhs <= width
        return (0, i * rhs) if packed else (i, 0)

    def to_sums(products, ref):
        for line in range(ref.shape[1]):
            spread = jnp.zeros((rhs, width), jnp.float32)
            for i, product in enumerate(products):
                at, shift = place(i, len(products))
                if at == line:
                    column = jnp.sum(product, axis=1, keepdims=True)
                    spread = jnp.where(lane_at == row_at + shift, column, spread)
            ref[0, line:line + 1, :] = jnp.sum(spread, axis=0, keepdims=True)

    def unpack(ref, i, count):
        at, shift = place(i, count)
        row = jnp.sum(ref[:, at, :], axis=0, keepdims=True)
        return jnp.sum(jnp.where(lane_at == row_at + shift, row, 0.0), axis=1, keepdims=True)

    def exchange(ref, send_sem, recv_sem):
        def send(k, carry):
            up, over = k // n_blk, k % n_blk
            peer = (lax.rem(own + up, n_own), lax.rem(blk + over, n_blk))
            slot = lax.rem(n_own - up, n_own) * n_blk + lax.rem(n_blk - over, n_blk)
            pltpu.make_async_remote_copy(
                src_ref=ref.at[0], dst_ref=ref.at[slot], send_sem=send_sem,
                recv_sem=recv_sem, device_id=peer, device_id_type=MESH).start()
            return carry

        lax.fori_loop(1, n_all, send, 0, unroll=n_all <= 64)

        def finish():
            wait_bytes(ref.at[pl.ds(1, n_all - 1)], send_sem)
            wait_bytes(ref.at[pl.ds(1, n_all - 1)], recv_sem)

        return finish

    residual = residual_ref[...]
    direction = direction_ref[...]
    to_sums([residual * residual], square_ref)

    for copy in row_copies:
        copy.wait_recv()
    chunk = math.gcd(n_row * width, 2 * width)
    n_chunk = n_row * width // chunk
    for c in range(n_chunk):
        wide = rows_ref[:, c * chunk:(c + 1) * chunk].astype(jnp.float32)
        norms_ref[:, c * chunk:(c + 1) * chunk] = jnp.sum(wide * wide, axis=0, keepdims=True) * scale

    part_copies = []
    per = chunk // width
    for k in range(n_col):
        if k > 0:
            wait_bytes(cols_ref.at[k], col_recv.at[k])
        wide = cols_ref[k, :dim, :].astype(jnp.float32).T
        col_norms = jnp.sum(wide * wide, axis=1, keepdims=True) * scale
        turned = wide.astype(jnp.bfloat16)
        dirs = cols_ref[k, dim:, :]
        for c in range(n_chunk):
            at = slice(c * chunk, (c + 1) * chunk)
            inner = jnp.dot(turned, rows_ref[:, at], preferred_element_type=jnp.float32)
            power = jnp.minimum(inner * (2.0 * scale) - norms_ref[:, at] - col_norms, 0.0)
            kern = (amplitude * jnp.exp2(power)).astype(jnp.bfloat16)
            value = jnp.dot(dirs, kern, preferred_element_type=jnp.float32)
            if k > 0:
                value += acc_ref[:, at]
            if k < n_col - 1:
                acc_ref[:, at] = value
                continue
            for j in range(per):
                to = c * per + j
                piece = value[:, j * width:(j + 1) * width]
                if to == 0:
                    acc_ref[:, :width] = piece
                    continue
                part_ref[to] = piece.astype(jnp.bfloat16)
                slot = n_row - to
                copy = pltpu.make_async_remote_copy(
                    src_ref=part_ref.at[to], dst_ref=back_ref.at[slot],
                    send_sem=part_send.at[slot], recv_sem=part_recv.at[slot],
                    device_id=row_peer(to), device_id_type=MESH)
                copy.start()
                part_copies.append(copy)

    early = exchange(square_ref, sum_send.at[1], sum_recv.at[1])
    image = acc_ref[:, :width]
    for k in range(1, n_row):
        wait_bytes(back_ref.at[k], part_recv.at[k])
        image += back_ref[k].astype(jnp.float32)
    image = image[:rhs] + noise_level * direction

    to_sums([direction * image, residual * image, image * image], sums_ref)
    late = exchange(sums_ref, sum_send.at[0], sum_recv.at[0])
    image_out[...] = image
    for copy in col_copies + row_copies + part_copies:
        copy.wait_send()
    early()
    late()
    rr = unpack(square_ref, 0, 1)
    pq, rq, qq = (unpack(sums_ref, i, 3) for i in range(3))
    alpha = rr / pq
    new_sum = rr - 2.0 * alpha * rq + alpha * alpha * qq
    alpha_out[...] = jnp.broadcast_to(alpha, (rhs, width))
    beta_out[...] = jnp.broadcast_to(new_sum / rr, (rhs, width))


def update(image, alpha, beta, solution_field, residual, direction, solution_out, residual_out, direction_out):
    residual_next = residual[...] - alpha[...] * image[...]
    residual_out[...] = residual_next
    solution_out[...] = solution_field[...] + alpha[...] * direction[...]
    direction_out[...] = residual_next + beta[...] * direction[...]


def local(n_own, n_blk, points, solution_field, residual, direction):
    low = split_own(n_own, n_blk)
    n_row, n_col = low * n_blk, n_own // low
    dim, width = points.shape
    rhs = direction.shape[0]
    padded = -(-rhs // 16) * 16
    vmem = pl.BlockSpec(memory_space=pltpu.VMEM)
    out = jax.ShapeDtypeStruct(direction.shape, jnp.float32)
    dma = pltpu.SemaphoreType.DMA
    image, alpha, beta = pl.pallas_call(
        functools.partial(kernel, n_own, n_blk, low),
        out_shape=(out, out, out),
        in_specs=[pl.BlockSpec(memory_space=pl.ANY)] * 3,
        out_specs=(vmem,) * 3,
        scratch_shapes=[
            pltpu.VMEM(points.shape, jnp.bfloat16),
            pltpu.VMEM(direction.shape, jnp.float32),
            pltpu.VMEM(direction.shape, jnp.float32),
            dma((3,)),
            pltpu.VMEM((dim, n_row * width), jnp.bfloat16),
            pltpu.VMEM((n_col, dim + padded, width), jnp.bfloat16),
            pltpu.VMEM((1, n_row * width), jnp.float32),
            pltpu.VMEM((padded, n_row * width), jnp.float32),
            pltpu.VMEM((n_row, padded, width), jnp.bfloat16),
            pltpu.VMEM((n_row, padded, width), jnp.bfloat16),
            pltpu.VMEM((n_own * n_blk, 1 if 3 * rhs <= width else 3, width), jnp.float32),
            pltpu.VMEM((n_own * n_blk, 1, width), jnp.float32),
            dma((n_row,)), dma((n_row,)), dma((n_col,)), dma((n_col,)),
            dma((n_row,)), dma((n_row,)), dma((2,)), dma((2,)),
        ],
        compiler_params=pltpu.CompilerParams(collective_id=0, has_side_effects=True),
    )(points, residual, direction)
    return pl.pallas_call(
        update, out_shape=(out, out, out), in_specs=[vmem] * 6, out_specs=(vmem,) * 3,
    )(image, alpha, beta, solution_field, residual, direction)


def solution(mesh):
    spec = P(None, ("own", "blk"))
    body = functools.partial(local, mesh.shape["own"], mesh.shape["blk"])
    return jax.shard_map(body, mesh=mesh, in_specs=(spec,) * 4, out_specs=(spec,) * 3, check_vma=False)
```

```python
import functools
import math

import jax
import jax.numpy as jnp
from jax import lax
from jax.experimental import pallas as pl
from jax.experimental.pallas import tpu as pltpu
from jax.sharding import PartitionSpec as P

amplitude = 1.0
decay_rate = 1.0 / 16.0
noise_level = 0.5

LOG2E = math.log2(math.e)
MESH = pl.DeviceIdType.MESH


def split_own(n_own, n_blk):
    for low in range(1, n_own + 1):
        if n_own % low == 0 and low * n_blk > n_own // low:
            return low
    return n_own


def wait_bytes(ref, sem):
    pltpu.make_async_copy(ref, ref, sem).wait()


def kernel(n_own, n_blk, low, points_hbm, residual_hbm, direction_hbm, image_out, alpha_out, beta_out,
           points_ref, residual_ref, direction_ref, load_sem, rows_ref, cols_ref, norms_ref, acc_ref, part_ref, back_ref, sums_ref, square_ref,
           row_send, row_recv, col_send, col_recv, part_send, part_recv, sum_send, sum_recv):
    high = n_own // low
    n_row, n_col = low * n_blk, high
    dim, width = points_ref.shape
    rhs = direction_ref.shape[0]
    loads = [
        pltpu.make_async_copy(points_hbm, points_ref, load_sem.at[0]),
        pltpu.make_async_copy(direction_hbm, direction_ref, load_sem.at[1]),
        pltpu.make_async_copy(residual_hbm, residual_ref, load_sem.at[2]),
    ]
    for load in loads:
        load.start()
    own, blk = lax.axis_index("own"), lax.axis_index("blk")
    h, l = lax.div(own, low), lax.rem(own, low)
    r = l * n_blk + blk
    scale = decay_rate * LOG2E

    def row_peer(k):
        other = lax.rem(r + k, n_row)
        return (h * low + lax.div(other, n_blk), lax.rem(other, n_blk))

    paired = n_col & (n_col - 1) == 0

    def col_peer(k):
        if not paired:
            return (lax.rem(h + k, high) * low + l, blk)
        other, bit = h, 1
        while bit <= k:
            if k & bit:
                other = other + bit - 2 * bit * lax.rem(lax.div(h, bit), 2)
            bit *= 2
        return (other * low + l, blk)

    barrier = pltpu.get_barrier_semaphore()
    for k in range(1, n_col):
        pl.semaphore_signal(barrier, inc=1, device_id=col_peer(k), device_id_type=MESH)
    for k in range(1, n_row):
        pl.semaphore_signal(barrier, inc=1, device_id=row_peer(k), device_id_type=MESH)

    for load in loads:
        load.wait()
    cols_ref[0, :dim, :] = points_ref[...]
    cols_ref[0, dim:, :] = jnp.zeros(cols_ref.shape[1:], jnp.bfloat16)[dim:]
    cols_ref[0, dim:dim + rhs, :] = direction_ref[...].astype(jnp.bfloat16)
    rows_ref[:, :width] = points_ref[...]

    pl.semaphore_wait(barrier, n_row + n_col - 2)

    col_copies = []
    for k in reversed(range(1, n_col)):
        slot = k if paired else n_col - k
        copy = pltpu.make_async_remote_copy(
            src_ref=cols_ref.at[0], dst_ref=cols_ref.at[slot], send_sem=col_send.at[slot],
            recv_sem=col_recv.at[slot], device_id=col_peer(k), device_id_type=MESH)
        copy.start()
        col_copies.append(copy)
    row_copies = []
    for k in range(1, n_row):
        slot = n_row - k
        copy = pltpu.make_async_remote_copy(
            src_ref=points_ref, dst_ref=rows_ref.at[:, pl.ds(slot * width, width)],
            send_sem=row_send.at[slot], recv_sem=row_recv.at[slot],
            device_id=row_peer(k), device_id_type=MESH)
        copy.start()
        row_copies.append(copy)

    row_at = lax.broadcasted_iota(jnp.int32, (rhs, width), 0)
    lane_at = lax.broadcasted_iota(jnp.int32, (rhs, width), 1)
    n_all = n_own * n_blk

    def place(i, count):
        packed = count * rhs <= width
        return (0, i * rhs) if packed else (i, 0)

    def to_sums(products, ref):
        for line in range(ref.shape[1]):
            spread = jnp.zeros((rhs, width), jnp.float32)
            for i, product in enumerate(products):
                at, shift = place(i, len(products))
                if at == line:
                    column = jnp.sum(product, axis=1, keepdims=True)
                    spread = jnp.where(lane_at == row_at + shift, column, spread)
            ref[0, line:line + 1, :] = jnp.sum(spread, axis=0, keepdims=True)

    def unpack(ref, i, count):
        at, shift = place(i, count)
        row = jnp.sum(ref[:, at, :], axis=0, keepdims=True)
        return jnp.sum(jnp.where(lane_at == row_at + shift, row, 0.0), axis=1, keepdims=True)

    def exchange(ref, send_sem, recv_sem):
        def send(k, carry):
            up, over = k // n_blk, k % n_blk
            peer = (lax.rem(own + up, n_own), lax.rem(blk + over, n_blk))
            slot = lax.rem(n_own - up, n_own) * n_blk + lax.rem(n_blk - over, n_blk)
            pltpu.make_async_remote_copy(
                src_ref=ref.at[0], dst_ref=ref.at[slot], send_sem=send_sem,
                recv_sem=recv_sem, device_id=peer, device_id_type=MESH).start()
            return carry

        lax.fori_loop(1, n_all, send, 0, unroll=n_all <= 64)

        def finish():
            wait_bytes(ref.at[pl.ds(1, n_all - 1)], send_sem)
            wait_bytes(ref.at[pl.ds(1, n_all - 1)], recv_sem)

        return finish

    residual = residual_ref[...]
    direction = direction_ref[...]
    to_sums([residual * residual], square_ref)

    for copy in row_copies:
        copy.wait_recv()
    chunk = math.gcd(n_row * width, 8 * width)
    n_chunk = n_row * width // chunk
    for c in range(n_chunk):
        wide = rows_ref[:, c * chunk:(c + 1) * chunk].astype(jnp.float32)
        norms_ref[:, c * chunk:(c + 1) * chunk] = jnp.sum(wide * wide, axis=0, keepdims=True) * scale

    part_copies = []
    per = chunk // width
    for k in range(n_col):
        if k > 0:
            wait_bytes(cols_ref.at[k], col_recv.at[k])
        wide = cols_ref[k, :dim, :].astype(jnp.float32).T
        col_norms = jnp.sum(wide * wide, axis=1, keepdims=True) * scale
        turned = wide.astype(jnp.bfloat16)
        dirs = cols_ref[k, dim:, :]
        for c in range(n_chunk):
            at = slice(c * chunk, (c + 1) * chunk)
            inner = jnp.dot(turned, rows_ref[:, at], preferred_element_type=jnp.float32)
            power = jnp.minimum(inner * (2.0 * scale) - norms_ref[:, at] - col_norms, 0.0)
            kern = (amplitude * jnp.exp2(power)).astype(jnp.bfloat16)
            value = jnp.dot(dirs, kern, preferred_element_type=jnp.float32)
            if k > 0:
                value += acc_ref[:, at]
            if k < n_col - 1:
                acc_ref[:, at] = value
                continue
            for j in range(per):
                to = c * per + j
                piece = value[:, j * width:(j + 1) * width]
                if to == 0:
                    acc_ref[:, :width] = piece
                    continue
                part_ref[to] = piece.astype(jnp.bfloat16)
                slot = n_row - to
                copy = pltpu.make_async_remote_copy(
                    src_ref=part_ref.at[to], dst_ref=back_ref.at[slot],
                    send_sem=part_send.at[slot], recv_sem=part_recv.at[slot],
                    device_id=row_peer(to), device_id_type=MESH)
                copy.start()
                part_copies.append(copy)

    early = exchange(square_ref, sum_send.at[1], sum_recv.at[1])
    image = acc_ref[:, :width]
    for k in range(1, n_row):
        wait_bytes(back_ref.at[k], part_recv.at[k])
        image += back_ref[k].astype(jnp.float32)
    image = image[:rhs] + noise_level * direction

    to_sums([direction * image, residual * image, image * image], sums_ref)
    late = exchange(sums_ref, sum_send.at[0], sum_recv.at[0])
    image_out[...] = image
    for copy in col_copies + row_copies + part_copies:
        copy.wait_send()
    early()
    late()
    rr = unpack(square_ref, 0, 1)
    pq, rq, qq = (unpack(sums_ref, i, 3) for i in range(3))
    alpha = rr / pq
    new_sum = rr - 2.0 * alpha * rq + alpha * alpha * qq
    alpha_out[...] = jnp.broadcast_to(alpha, (rhs, width))
    beta_out[...] = jnp.broadcast_to(new_sum / rr, (rhs, width))


def update(image, alpha, beta, solution_field, residual, direction, solution_out, residual_out, direction_out):
    residual_next = residual[...] - alpha[...] * image[...]
    residual_out[...] = residual_next
    solution_out[...] = solution_field[...] + alpha[...] * direction[...]
    direction_out[...] = residual_next + beta[...] * direction[...]


def local(n_own, n_blk, points, solution_field, residual, direction):
    low = split_own(n_own, n_blk)
    n_row, n_col = low * n_blk, n_own // low
    dim, width = points.shape
    rhs = direction.shape[0]
    padded = -(-rhs // 16) * 16
    vmem = pl.BlockSpec(memory_space=pltpu.VMEM)
    out = jax.ShapeDtypeStruct(direction.shape, jnp.float32)
    dma = pltpu.SemaphoreType.DMA
    image, alpha, beta = pl.pallas_call(
        functools.partial(kernel, n_own, n_blk, low),
        out_shape=(pltpu.VMEM(direction.shape, jnp.float32),) * 3,
        in_specs=[pl.BlockSpec(memory_space=pl.ANY)] * 3,
        out_specs=(vmem,) * 3,
        scratch_shapes=[
            pltpu.VMEM(points.shape, jnp.bfloat16),
            pltpu.VMEM(direction.shape, jnp.float32),
            pltpu.VMEM(direction.shape, jnp.float32),
            dma((3,)),
            pltpu.VMEM((dim, n_row * width), jnp.bfloat16),
            pltpu.VMEM((n_col, dim + padded, width), jnp.bfloat16),
            pltpu.VMEM((1, n_row * width), jnp.float32),
            pltpu.VMEM((padded, n_row * width), jnp.float32),
            pltpu.VMEM((n_row, padded, width), jnp.bfloat16),
            pltpu.VMEM((n_row, padded, width), jnp.bfloat16),
            pltpu.VMEM((n_own * n_blk, 1 if 3 * rhs <= width else 3, width), jnp.float32),
            pltpu.VMEM((n_own * n_blk, 1, width), jnp.float32),
            dma((n_row,)), dma((n_row,)), dma((n_col,)), dma((n_col,)),
            dma((n_row,)), dma((n_row,)), dma((2,)), dma((2,)),
        ],
        compiler_params=pltpu.CompilerParams(collective_id=0, has_side_effects=True),
    )(points, residual, direction)
    residual_next = residual - alpha * image
    return solution_field + alpha * direction, residual_next, residual_next + beta * direction


def solution(mesh):
    spec = P(None, ("own", "blk"))
    body = functools.partial(local, mesh.shape["own"], mesh.shape["blk"])
    return jax.shard_map(body, mesh=mesh, in_specs=(spec,) * 4, out_specs=(spec,) * 3, check_vma=False)
```

```python
import functools
import math

import jax
import jax.numpy as jnp
from jax import lax
from jax.experimental import pallas as pl
from jax.experimental.pallas import tpu as pltpu
from jax.sharding import PartitionSpec as P

amplitude = 1.0
decay_rate = 1.0 / 16.0
noise_level = 0.5

LOG2E = math.log2(math.e)
MESH = pl.DeviceIdType.MESH


def split_own(n_own, n_blk):
    for low in range(1, n_own + 1):
        if n_own % low == 0 and low * n_blk > n_own // low:
            return low
    return n_own


def wait_bytes(ref, sem):
    pltpu.make_async_copy(ref, ref, sem).wait()


def kernel(n_own, n_blk, low, points_hbm, residual_hbm, direction_hbm, image_out, alpha_out, beta_out,
           points_ref, residual_ref, direction_ref, load_sem, rows_ref, cols_ref, norms_ref, acc_ref, part_ref, back_ref, sums_ref,
           row_send, row_recv, col_send, col_recv, part_send, part_recv, sum_send, sum_recv):
    high = n_own // low
    n_row, n_col = low * n_blk, high
    dim, width = points_ref.shape
    rhs = direction_ref.shape[0]
    loads = [
        pltpu.make_async_copy(points_hbm, points_ref, load_sem.at[0]),
        pltpu.make_async_copy(direction_hbm, direction_ref, load_sem.at[1]),
        pltpu.make_async_copy(residual_hbm, residual_ref, load_sem.at[2]),
    ]
    for load in loads:
        load.start()
    own, blk = lax.axis_index("own"), lax.axis_index("blk")
    h, l = lax.div(own, low), lax.rem(own, low)
    r = l * n_blk + blk
    scale = decay_rate * LOG2E

    def row_peer(k):
        other = lax.rem(r + k, n_row)
        return (h * low + lax.div(other, n_blk), lax.rem(other, n_blk))

    paired = n_col & (n_col - 1) == 0

    def col_peer(k):
        if not paired:
            return (lax.rem(h + k, high) * low + l, blk)
        other, bit = h, 1
        while bit <= k:
            if k & bit:
                other = other + bit - 2 * bit * lax.rem(lax.div(h, bit), 2)
            bit *= 2
        return (other * low + l, blk)

    barrier = pltpu.get_barrier_semaphore()
    for k in range(1, n_col):
        pl.semaphore_signal(barrier, inc=1, device_id=col_peer(k), device_id_type=MESH)
    for k in range(1, n_row):
        pl.semaphore_signal(barrier, inc=1, device_id=row_peer(k), device_id_type=MESH)

    for load in loads[:2]:
        load.wait()
    cols_ref[0, :dim, :] = points_ref[...]
    cols_ref[0, dim:, :] = jnp.zeros(cols_ref.shape[1:], jnp.bfloat16)[dim:]
    cols_ref[0, dim:dim + rhs, :] = direction_ref[...].astype(jnp.bfloat16)
    rows_ref[:, :width] = points_ref[...]

    pl.semaphore_wait(barrier, n_row + n_col - 2)

    col_copies = []
    for k in reversed(range(1, n_col)):
        slot = k if paired else n_col - k
        copy = pltpu.make_async_remote_copy(
            src_ref=cols_ref.at[0], dst_ref=cols_ref.at[slot], send_sem=col_send.at[slot],
            recv_sem=col_recv.at[slot], device_id=col_peer(k), device_id_type=MESH)
        copy.start()
        col_copies.append(copy)
    row_copies = []
    for k in range(1, n_row):
        slot = n_row - k
        copy = pltpu.make_async_remote_copy(
            src_ref=points_ref, dst_ref=rows_ref.at[:, pl.ds(slot * width, width)],
            send_sem=row_send.at[slot], recv_sem=row_recv.at[slot],
            device_id=row_peer(k), device_id_type=MESH)
        copy.start()
        row_copies.append(copy)

    row_at = lax.broadcasted_iota(jnp.int32, (rhs, width), 0)
    lane_at = lax.broadcasted_iota(jnp.int32, (rhs, width), 1)
    n_all = n_own * n_blk

    def place(i, count):
        per_line = max(1, width // rhs)
        return (i // per_line, i % per_line * rhs)

    def to_sums(products, ref):
        for line in range(ref.shape[1]):
            spread = jnp.zeros((rhs, width), jnp.float32)
            for i, product in enumerate(products):
                at, shift = place(i, len(products))
                if at == line:
                    column = jnp.sum(product, axis=1, keepdims=True)
                    spread = jnp.where(lane_at == row_at + shift, column, spread)
            ref[0, line:line + 1, :] = jnp.sum(spread, axis=0, keepdims=True)

    def unpack(ref, i, count):
        at, shift = place(i, count)
        row = jnp.sum(ref[:, at, :], axis=0, keepdims=True)
        return jnp.sum(jnp.where(lane_at == row_at + shift, row, 0.0), axis=1, keepdims=True)

    def exchange(ref, send_sem, recv_sem):
        def send(k, carry):
            up, over = k // n_blk, k % n_blk
            peer = (lax.rem(own + up, n_own), lax.rem(blk + over, n_blk))
            slot = lax.rem(n_own - up, n_own) * n_blk + lax.rem(n_blk - over, n_blk)
            pltpu.make_async_remote_copy(
                src_ref=ref.at[0], dst_ref=ref.at[slot], send_sem=send_sem,
                recv_sem=recv_sem, device_id=peer, device_id_type=MESH).start()
            return carry

        lax.fori_loop(1, n_all, send, 0, unroll=n_all <= 64)

        def finish():
            wait_bytes(ref.at[pl.ds(1, n_all - 1)], send_sem)
            wait_bytes(ref.at[pl.ds(1, n_all - 1)], recv_sem)

        return finish

    loads[2].wait()
    residual = residual_ref[...]
    direction = direction_ref[...]

    for copy in row_copies:
        copy.wait_recv()
    chunk = math.gcd(n_row * width, 8 * width)
    n_chunk = n_row * width // chunk
    for c in range(n_chunk):
        wide = rows_ref[:, c * chunk:(c + 1) * chunk].astype(jnp.float32)
        norms_ref[:, c * chunk:(c + 1) * chunk] = jnp.sum(wide * wide, axis=0, keepdims=True) * scale

    part_copies = []
    per = chunk // width
    for k in range(n_col):
        if k > 0:
            wait_bytes(cols_ref.at[k], col_recv.at[k])
        wide = cols_ref[k, :dim, :].astype(jnp.float32).T
        col_norms = jnp.sum(wide * wide, axis=1, keepdims=True) * scale
        turned = wide.astype(jnp.bfloat16)
        dirs = cols_ref[k, dim:, :]
        for c in range(n_chunk):
            at = slice(c * chunk, (c + 1) * chunk)
            inner = jnp.dot(turned, rows_ref[:, at], preferred_element_type=jnp.float32)
            power = jnp.minimum(inner * (2.0 * scale) - norms_ref[:, at] - col_norms, 0.0)
            kern = (amplitude * jnp.exp2(power)).astype(jnp.bfloat16)
            value = jnp.dot(dirs, kern, preferred_element_type=jnp.float32)
            if k > 0:
                value += acc_ref[:, at]
            if k < n_col - 1:
                acc_ref[:, at] = value
                continue
            for j in range(per):
                to = c * per + j
                piece = value[:, j * width:(j + 1) * width]
                if to == 0:
                    acc_ref[:, :width] = piece
                    continue
                part_ref[to] = piece.astype(jnp.bfloat16)
                slot = n_row - to
                copy = pltpu.make_async_remote_copy(
                    src_ref=part_ref.at[to], dst_ref=back_ref.at[slot],
                    send_sem=part_send.at[slot], recv_sem=part_recv.at[slot],
                    device_id=row_peer(to), device_id_type=MESH)
                copy.start()
                part_copies.append(copy)

    image = acc_ref[:, :width]
    for k in range(1, n_row):
        wait_bytes(back_ref.at[k], part_recv.at[k])
        image += back_ref[k].astype(jnp.float32)
    image = image[:rhs] + noise_level * direction

    to_sums([residual * residual, direction * image, residual * image, image * image], sums_ref)
    late = exchange(sums_ref, sum_send.at[0], sum_recv.at[0])
    image_out[...] = image
    for copy in col_copies + row_copies + part_copies:
        copy.wait_send()
    late()
    rr, pq, rq, qq = (unpack(sums_ref, i, 4) for i in range(4))
    alpha = rr / pq
    new_sum = rr - 2.0 * alpha * rq + alpha * alpha * qq
    alpha_out[...] = jnp.broadcast_to(alpha, (rhs, width))
    beta_out[...] = jnp.broadcast_to(new_sum / rr, (rhs, width))


def update(image, alpha, beta, solution_field, residual, direction, solution_out, residual_out, direction_out):
    residual_next = residual[...] - alpha[...] * image[...]
    residual_out[...] = residual_next
    solution_out[...] = solution_field[...] + alpha[...] * direction[...]
    direction_out[...] = residual_next + beta[...] * direction[...]


def local(n_own, n_blk, points, solution_field, residual, direction):
    low = split_own(n_own, n_blk)
    n_row, n_col = low * n_blk, n_own // low
    dim, width = points.shape
    rhs = direction.shape[0]
    padded = -(-rhs // 8) * 8
    vmem = pl.BlockSpec(memory_space=pltpu.VMEM)
    out = jax.ShapeDtypeStruct(direction.shape, jnp.float32)
    dma = pltpu.SemaphoreType.DMA
    image, alpha, beta = pl.pallas_call(
        functools.partial(kernel, n_own, n_blk, low),
        out_shape=(pltpu.VMEM(direction.shape, jnp.float32),) * 3,
        in_specs=[pl.BlockSpec(memory_space=pl.ANY)] * 3,
        out_specs=(vmem,) * 3,
        scratch_shapes=[
            pltpu.VMEM(points.shape, jnp.bfloat16),
            pltpu.VMEM(direction.shape, jnp.float32),
            pltpu.VMEM(direction.shape, jnp.float32),
            dma((3,)),
            pltpu.VMEM((dim, n_row * width), jnp.bfloat16),
            pltpu.VMEM((n_col, dim + padded, width), jnp.bfloat16),
            pltpu.VMEM((1, n_row * width), jnp.float32),
            pltpu.VMEM((padded, n_row * width), jnp.float32),
            pltpu.VMEM((n_row, padded, width), jnp.bfloat16),
            pltpu.VMEM((n_row, padded, width), jnp.bfloat16),
            pltpu.VMEM((n_own * n_blk, -(-4 // max(1, width // rhs)), width), jnp.float32),
            dma((n_row,)), dma((n_row,)), dma((n_col,)), dma((n_col,)),
            dma((n_row,)), dma((n_row,)), dma((1,)), dma((1,)),
        ],
        compiler_params=pltpu.CompilerParams(collective_id=0, has_side_effects=True),
    )(points, residual, direction)
    residual_next = residual - alpha * image
    return solution_field + alpha * direction, residual_next, residual_next + beta * direction


def solution(mesh):
    spec = P(None, ("own", "blk"))
    body = functools.partial(local, mesh.shape["own"], mesh.shape["blk"])
    return jax.shard_map(body, mesh=mesh, in_specs=(spec,) * 4, out_specs=(spec,) * 3, check_vma=False)
```
